128 devices in a mesh: dp: 64 (over z, y, x), cp: 2 (over core).
Axes of the slice: x: 4, y: 4, z: 4, core: 2. Of those that a mesh axis runs over, the one named last changes fastest.
Arguments:
- hidden_states: bfloat16 [64, 512, 3072], P('dp', 'cp')
- norm_gain: float32 [3072], replicated
- w_gate: bfloat16 [3072, 8192], replicated
- w_up: bfloat16 [3072, 8192], replicated
- w_down: bfloat16 [8192, 3072], replicated
- final_gain: float32 [3072], replicated
- w_value: float32 [3072], replicated
- b_value: float32 [], replicated
- rewards: float32 [64, 512], P('dp', 'cp')
- mask: int32 [64, 512], P('dp', 'cp')
Outputs:
- output 1: float32 [64, 512], P('dp', 'cp')
- output 2: float32 [64, 512], P('dp', 'cp')
- output 3: float32 [64, 512], P('dp', 'cp')
All inputs are finite; a program needn't handle non-finite values.
Results may differ from the reference program's by a relative error of at most 0.001.
Values sent between devices are 32-bit elements.
A program may use at most 1 GiB of HBM per device.

```python
import jax
import jax.numpy as jnp
from jax import lax

ROW_COUNT = 64
SEQ_LEN = 512
MODEL_DIM = 3072
FFN_DIM = 8192
NORM_EPS = 1e-6
WHITEN_EPS = 1e-8
DISCOUNT = 1.0
GAE_LAMBDA = 0.995


def draw_mask(start_key, end_key):
    starts = jax.random.randint(start_key, (ROW_COUNT,), 0, SEQ_LEN // 2)
    ends = starts + jax.random.randint(end_key, (ROW_COUNT,), 0, SEQ_LEN - starts)
    positions = jnp.arange(SEQ_LEN)[None, :]
    inside = (positions >= starts[:, None]) & (positions <= ends[:, None])
    return inside.astype(jnp.int32), ends


def setup_inputs(seed: int = 0) -> dict:
    keys = jax.random.split(jax.random.key(seed), 12)
    hidden_states = jax.random.normal(keys[0], (ROW_COUNT, SEQ_LEN, MODEL_DIM), jnp.float32).astype(jnp.bfloat16)
    norm_gain = 1.0 + 0.3 * jax.random.normal(keys[1], (MODEL_DIM,), jnp.float32)
    w_gate = (jax.random.normal(keys[2], (MODEL_DIM, FFN_DIM), jnp.float32) * MODEL_DIM ** -0.5).astype(jnp.bfloat16)
    w_up = (jax.random.normal(keys[3], (MODEL_DIM, FFN_DIM), jnp.float32) * MODEL_DIM ** -0.5).astype(jnp.bfloat16)
    w_down = (jax.random.normal(keys[4], (FFN_DIM, MODEL_DIM), jnp.float32) * FFN_DIM ** -0.5).astype(jnp.bfloat16)
    final_gain = 1.0 + 0.3 * jax.random.normal(keys[5], (MODEL_DIM,), jnp.float32)
    w_value = jax.random.normal(keys[6], (MODEL_DIM,), jnp.float32) * MODEL_DIM ** -0.5
    b_value = jax.random.uniform(keys[7], (), jnp.float32, 0.5, 1.0)
    mask, ends = draw_mask(keys[8], keys[9])
    shaping = 0.05 * jax.random.normal(keys[10], (ROW_COUNT, SEQ_LEN), jnp.float32)
    score = 2.0 * jax.random.normal(keys[11], (ROW_COUNT,), jnp.float32)
    at_end = jnp.arange(SEQ_LEN)[None, :] == ends[:, None]
    rewards = shaping + jnp.where(at_end, score[:, None], 0.0)
    return dict(hidden_states=hidden_states, norm_gain=norm_gain, w_gate=w_gate, w_up=w_up, w_down=w_down, final_gain=final_gain, w_value=w_value, b_value=b_value, rewards=rewards, mask=mask)


def reference(hidden_states, norm_gain, w_gate, w_up, w_down, final_gain, w_value, b_value, rewards, mask):
    head_vec = final_gain * w_value

    def row_value(x_row):
        x_f32 = x_row.astype(jnp.float32)
        normed = (x_f32 * lax.rsqrt(jnp.mean(x_f32 * x_f32, axis=-1, keepdims=True) + NORM_EPS) * norm_gain).astype(jnp.bfloat16)
        gate = jnp.dot(normed, w_gate, preferred_element_type=jnp.float32)
        up_val = jnp.dot(normed, w_up, preferred_element_type=jnp.float32)
        hidden = (jax.nn.silu(gate) * up_val).astype(jnp.bfloat16)
        resid = x_f32 + jnp.dot(hidden, w_down, preferred_element_type=jnp.float32)
        resid_n = resid * lax.rsqrt(jnp.mean(resid * resid, axis=-1, keepdims=True) + NORM_EPS)
        return jnp.sum(resid_n * head_vec, axis=-1) + b_value

    mask_f = mask.astype(jnp.float32)
    values = mask_f * lax.map(row_value, hidden_states)
    rew_masked = mask_f * rewards
    next_vals = jnp.concatenate([values[:, 1:], jnp.zeros_like(values[:, :1])], axis=1)
    delta = rew_masked + DISCOUNT * next_vals - values

    def back_step(carry, delta_col):
        adv_col = delta_col + DISCOUNT * GAE_LAMBDA * carry
        return adv_col, adv_col

    _, adv_cols = lax.scan(back_step, jnp.zeros_like(delta[:, 0]), delta.T, reverse=True)
    advantage = adv_cols.T
    count = jnp.sum(mask_f)
    mean_adv = jnp.sum(mask_f * advantage) / count
    var_adv = jnp.sum(mask_f * advantage * advantage) / count - mean_adv * mean_adv
    white = mask_f * (advantage - mean_adv) * lax.rsqrt(var_adv + WHITEN_EPS)
    return values, mask_f * (advantage + values), white
```

```python
import functools
import math

import jax
import jax.numpy as jnp
from jax import lax
from jax.experimental import pallas as pl
from jax.experimental.pallas import tpu as pltpu
from jax.sharding import PartitionSpec as P

NORM_EPS = 1e-6
WHITEN_EPS = 1e-8
DISCOUNT = 1.0
GAE_LAMBDA = 0.995
DECAY = DISCOUNT * GAE_LAMBDA
LOG_DECAY = math.log(DECAY)
MESH = pl.DeviceIdType.MESH


def critic_values(x_blk, norm_gain, w_gate, w_up, w_down, final_gain, w_value, b_value):
    x_f32 = x_blk.astype(jnp.float32)
    normed = (x_f32 * lax.rsqrt(jnp.mean(x_f32 * x_f32, axis=-1, keepdims=True) + NORM_EPS) * norm_gain).astype(jnp.bfloat16)
    gate = jnp.einsum('bsd,df->bsf', normed, w_gate, preferred_element_type=jnp.float32)
    up_val = jnp.einsum('bsd,df->bsf', normed, w_up, preferred_element_type=jnp.float32)
    hidden = (jax.nn.silu(gate) * up_val).astype(jnp.bfloat16)
    resid = x_f32 + jnp.einsum('bsf,fd->bsd', hidden, w_down, preferred_element_type=jnp.float32)
    resid_n = resid * lax.rsqrt(jnp.mean(resid * resid, axis=-1, keepdims=True) + NORM_EPS)
    return jnp.sum(resid_n * (final_gain * w_value), axis=-1) + b_value


def greet(dp_size):
    chip, core = lax.axis_index("dp"), lax.axis_index("cp")
    barrier = pltpu.get_barrier_semaphore()
    pl.semaphore_signal(barrier, inc=1, device_id=(chip, 1 - core), device_id_type=MESH)

    def tell(k, _):
        pl.semaphore_signal(barrier, inc=1, device_id=(lax.rem(chip + k, dp_size), core), device_id_type=MESH)
        return 0

    lax.fori_loop(1, dp_size, tell, 0)


def await_greetings(dp_size):
    pl.semaphore_wait(pltpu.get_barrier_semaphore(), dp_size)


def positions(n):
    row = lax.broadcasted_iota(jnp.int32, (n, n), 0)
    col = lax.broadcasted_iota(jnp.int32, (n, n), 1)
    return row, col


def column_of(row_vec, n):
    row, col = positions(n)
    return jnp.sum(jnp.where(row == col, row_vec, 0.0), axis=1, keepdims=True)


def reward_part(rew_col, n):
    row, col = positions(n)
    gap = row - col
    decay = jnp.where(gap >= 0, jnp.exp(jnp.maximum(gap, 0).astype(jnp.float32) * LOG_DECAY), 0.0)
    return jnp.sum(decay * rew_col, axis=0, keepdims=True)


def value_weights(n):
    row, col = positions(n)
    gap = row - col
    later = DISCOUNT * (1.0 - GAE_LAMBDA) * jnp.exp(jnp.maximum(gap - 1, 0).astype(jnp.float32) * LOG_DECAY)
    return jnp.where(gap > 0, later, jnp.where(gap == 0, -1.0, 0.0))


def finish(dp_size, v_col, reward_row, weights, mask_row, values_ref, returns_ref, white_ref,
           mine, theirs, total, gathered, pair_send, pair_recv, all_send, all_recv):
    n = mask_row.shape[1]
    chip, core = lax.axis_index("dp"), lax.axis_index("cp")
    row, col = positions(n)
    adv = reward_row + jnp.sum(weights * v_col, axis=0, keepdims=True)
    v_row = jnp.sum(jnp.where(row == col, v_col, 0.0), axis=0, keepdims=True)
    ahead = (n - 1) - lax.broadcasted_iota(jnp.int32, (1, n), 1)
    reach = jnp.exp(ahead.astype(jnp.float32) * LOG_DECAY)
    madv, mreach = mask_row * adv, mask_row * reach

    def add_up(a):
        return jnp.sum(a, axis=1, keepdims=True)

    carry_out = DISCOUNT * v_row[:, 0:1] + DECAY * adv[:, 0:1]
    parts = [add_up(mask_row), add_up(madv), add_up(madv * adv), add_up(mreach), add_up(mreach * adv), add_up(mreach * reach), carry_out]
    lane = lax.broadcasted_iota(jnp.int32, (1, 128), 1)
    packed = jnp.zeros((1, 128), jnp.float32)
    for place, part in enumerate(parts):
        packed = jnp.where(lane == place, part, packed)
    mine[...] = packed
    pair = pltpu.make_async_remote_copy(src_ref=mine, dst_ref=theirs, send_sem=pair_send, recv_sem=pair_recv,
                                        device_id=(chip, 1 - core), device_id_type=MESH)
    pair.start()
    pair.wait()
    other = theirs[...]
    is_left = core == 0
    left, right = jnp.where(is_left, packed, other), jnp.where(is_left, other, packed)
    carry = right[:, 6:7]
    count = left[:, 0:1] + right[:, 0:1]
    first = left[:, 1:2] + right[:, 1:2] + carry * left[:, 3:4]
    second = left[:, 2:3] + right[:, 2:3] + carry * (2.0 * left[:, 4:5] + carry * left[:, 5:6])
    own = jnp.where(lane == 0, count, jnp.where(lane == 1, first, jnp.where(lane == 2, second, 0.0)))
    total[...] = own

    def push(k, _):
        pltpu.make_async_remote_copy(
            src_ref=total, dst_ref=gathered.at[pl.ds(k - 1, 1)], send_sem=all_send, recv_sem=all_recv,
            device_id=(lax.rem(chip + k, dp_size), core), device_id_type=MESH).start()
        return 0

    lax.fori_loop(1, dp_size, push, 0)
    adv = adv + jnp.where(is_left, carry, 0.0) * reach
    values_ref[...] = v_row
    returns_ref[...] = mask_row * (adv + v_row)
    everything = pltpu.make_async_remote_copy(src_ref=gathered, dst_ref=gathered, send_sem=all_send, recv_sem=all_recv,
                                              device_id=(chip, 1 - core), device_id_type=MESH)
    everything.wait_recv()
    sums = own + jnp.sum(gathered[...], axis=0, keepdims=True)
    count, first, second = sums[:, 0:1], sums[:, 1:2], sums[:, 2:3]
    mean = first / count
    var = second / count - mean * mean
    white_ref[...] = mask_row * (adv - mean) * lax.rsqrt(var + WHITEN_EPS)
    everything.wait_send()


def tail_kernel(dp_size, v_ref, rew_ref, mask_ref, values_ref, returns_ref, white_ref, *scratch):
    n = v_ref.shape[1]
    greet(dp_size)
    mask_row = mask_ref[...].astype(jnp.float32)
    reward_row = reward_part(column_of(mask_row * rew_ref[...], n), n)
    v_col = column_of(mask_row * v_ref[...], n)
    await_greetings(dp_size)
    finish(dp_size, v_col, reward_row, value_weights(n), mask_row, values_ref, returns_ref, white_ref, *scratch)


def finish_scratch(dp_size):
    return [
        pltpu.VMEM((1, 128), jnp.float32),
        pltpu.VMEM((1, 128), jnp.float32),
        pltpu.VMEM((1, 128), jnp.float32),
        pltpu.VMEM((dp_size - 1, 128), jnp.float32),
        pltpu.SemaphoreType.DMA,
        pltpu.SemaphoreType.DMA,
        pltpu.SemaphoreType.DMA,
        pltpu.SemaphoreType.DMA,
    ]


def solution(mesh):
    dp_size = mesh.shape['dp']

    def local_step(x_blk, norm_gain, w_gate, w_up, w_down, final_gain, w_value, b_value, rew_blk, mask_blk):
        v = critic_values(x_blk, norm_gain, w_gate, w_up, w_down, final_gain, w_value, b_value)
        row = jax.ShapeDtypeStruct(rew_blk.shape, jnp.float32)
        vmem = pl.BlockSpec(memory_space=pltpu.VMEM)
        return pl.pallas_call(
            functools.partial(tail_kernel, dp_size),
            out_shape=(row, row, row),
            in_specs=[vmem] * 3,
            out_specs=(vmem,) * 3,
            scratch_shapes=finish_scratch(dp_size),
            compiler_params=pltpu.CompilerParams(collective_id=0, has_side_effects=True),
        )(v, rew_blk, mask_blk)

    tok_spec = P('dp', 'cp')
    in_specs = (P('dp', 'cp', None), P(None), P(None, None), P(None, None), P(None, None), P(None), P(None), P(), tok_spec, tok_spec)
    return jax.shard_map(local_step, mesh=mesh, in_specs=in_specs, out_specs=(tok_spec, tok_spec, tok_spec), check_vma=False)
```

```python
import functools
import math

import jax
import jax.numpy as jnp
from jax import lax
from jax.experimental import pallas as pl
from jax.experimental.pallas import tpu as pltpu
from jax.sharding import PartitionSpec as P

NORM_EPS = 1e-6
WHITEN_EPS = 1e-8
DISCOUNT = 1.0
GAE_LAMBDA = 0.995
DECAY = DISCOUNT * GAE_LAMBDA
LOG_DECAY = math.log(DECAY)
MESH = pl.DeviceIdType.MESH


TILE = 256
WIDE = 512
DEPTH2 = 2048
S1, S2 = 4, 8
NT = 512


def silu_mul(g, u):
    return (g * (1.0 / (1.0 + jnp.exp(-g))) * u).astype(jnp.bfloat16)


def mlp(x_hbm, wg_hbm, wu_hbm, wd_hbm, g2_ref, gf_ref, wv_ref,
        x_buf, n_buf, u_buf, wg_ring, wu_ring, wd_ring, sq_acc, hd_acc, h_buf, x_sem, g_sem, u_sem, d_sem, while_loading):
    rows, model = x_buf.shape
    ffn = u_buf.shape[1]
    n1 = ffn // WIDE
    per_out = ffn // DEPTH2
    n_out = model // WIDE
    n2 = n_out * per_out
    k1, k2 = model // TILE, DEPTH2 // TILE

    def g_copy(i):
        s = lax.rem(i, S1)
        return pltpu.make_async_copy(wg_hbm.at[:, pl.ds(pl.multiple_of(i * WIDE, WIDE), WIDE)], wg_ring.at[s], g_sem.at[s])

    def u_copy(i):
        s = lax.rem(i, S1)
        return pltpu.make_async_copy(wu_hbm.at[:, pl.ds(pl.multiple_of(i * WIDE, WIDE), WIDE)], wu_ring.at[s], u_sem.at[s])

    def d_copy(p):
        s = lax.rem(p, S2)
        o, kk = p // per_out, lax.rem(p, per_out)
        return pltpu.make_async_copy(
            wd_hbm.at[pl.ds(pl.multiple_of(kk * DEPTH2, DEPTH2), DEPTH2), pl.ds(pl.multiple_of(o * WIDE, WIDE), WIDE)],
            wd_ring.at[s], d_sem.at[s])

    x_copy = pltpu.make_async_copy(x_hbm, x_buf, x_sem)
    x_copy.start()
    for i in range(S1):
        g_copy(i).start()
        u_copy(i).start()
    while_loading()
    x_copy.wait()

    def norm(b, _):
        r = pl.ds(pl.multiple_of(b * 32, 32), 32)
        xf = x_buf[r, :].astype(jnp.float32)
        scale = lax.rsqrt(jnp.mean(xf * xf, axis=1, keepdims=True) + NORM_EPS)
        n_buf[r, :] = (xf * scale * g2_ref[...]).astype(jnp.bfloat16)
        return 0
    lax.fori_loop(0, rows // 32, norm, 0)
    sq_acc[...] = jnp.zeros_like(sq_acc)
    hd_acc[...] = jnp.zeros_like(hd_acc)

    def dot(a, b):
        return jnp.dot(a, b, preferred_element_type=jnp.float32)

    def issue1(i):
        @pl.when(i + S1 < n1)
        def _():
            g_copy(i + S1).start()
            u_copy(i + S1).start()

        @pl.when(i + S1 >= n1)
        def _():
            first = (i + S1 - n1) * (S2 // S1)
            for j in range(S2 // S1):
                d_copy(first + j).start()

    UN = 2
    def loop1(b, _):
        for j in range(UN):
            i = b * UN + j
            slot = lax.rem(i, S1)
            g_copy(i).wait()
            u_copy(i).wait()
            for half in range(WIDE // NT):
                c = pl.ds(half * NT, NT)
                g = dot(n_buf[...], wg_ring[slot, :, c])
                u = dot(n_buf[...], wu_ring[slot, :, c])
                u_buf[:, pl.ds(pl.multiple_of(i * WIDE + half * NT, NT), NT)] = silu_mul(g, u)
        for j in range(UN):
            issue1(b * UN + j)
        return 0
    lax.fori_loop(0, n1 // UN, loop1, 0)

    def loop2(o, _):
        h = None
        for kk in range(per_out):
            p = o * per_out + kk
            slot = lax.rem(p, S2)
            d_copy(p).wait()
            part = dot(u_buf[:, pl.ds(kk * DEPTH2, DEPTH2)], wd_ring[slot])
            if kk == 0:
                h_buf[...] = part
            elif kk < per_out - 1:
                h_buf[...] += part
            else:
                for q in range(4):
                    c = pl.ds(pl.multiple_of(o * WIDE + q * 128, 128), 128)
                    h = x_buf[:, c].astype(jnp.float32) + (h_buf[:, q*128:(q+1)*128] + part[:, q*128:(q+1)*128])
                    sq_acc[...] += h * h
                    hd_acc[...] += h * (gf_ref[:, c] * wv_ref[:, c])
            @pl.when(p + S2 < n2)
            def _():
                d_copy(p + S2).start()
        return 0
    lax.fori_loop(0, n_out, loop2, 0)


def greet(dp_size):
    chip, core = lax.axis_index("dp"), lax.axis_index("cp")
    barrier = pltpu.get_barrier_semaphore()
    pl.semaphore_signal(barrier, inc=1, device_id=(chip, 1 - core), device_id_type=MESH)

    def tell(k, _):
        pl.semaphore_signal(barrier, inc=1, device_id=(lax.rem(chip + k, dp_size), core), device_id_type=MESH)
        return 0

    lax.fori_loop(1, dp_size, tell, 0)


def await_greetings(dp_size):
    pl.semaphore_wait(pltpu.get_barrier_semaphore(), dp_size)


def positions(n):
    row = lax.broadcasted_iota(jnp.int32, (n, n), 0)
    col = lax.broadcasted_iota(jnp.int32, (n, n), 1)
    return row, col


def column_of(row_vec, n):
    row, col = positions(n)
    return jnp.sum(jnp.where(row == col, row_vec, 0.0), axis=1, keepdims=True)


def reward_part(rew_col, n):
    row, col = positions(n)
    gap = row - col
    decay = jnp.where(gap >= 0, jnp.exp(jnp.maximum(gap, 0).astype(jnp.float32) * LOG_DECAY), 0.0)
    return jnp.sum(decay * rew_col, axis=0, keepdims=True)


def value_weights(n):
    row, col = positions(n)
    gap = row - col
    later = DISCOUNT * (1.0 - GAE_LAMBDA) * jnp.exp(jnp.maximum(gap - 1, 0).astype(jnp.float32) * LOG_DECAY)
    return jnp.where(gap > 0, later, jnp.where(gap == 0, -1.0, 0.0))


def finish(dp_size, v_col, reward_row, weights, mask_row, out_ref,
           mine, theirs, total, gathered, pair_send, pair_recv, all_send, all_recv):
    n = mask_row.shape[1]
    chip, core = lax.axis_index("dp"), lax.axis_index("cp")
    row, col = positions(n)
    adv = reward_row + jnp.sum(weights * v_col, axis=0, keepdims=True)
    v_row = jnp.sum(jnp.where(row == col, v_col, 0.0), axis=0, keepdims=True)
    ahead = (n - 1) - lax.broadcasted_iota(jnp.int32, (1, n), 1)
    reach = jnp.exp(ahead.astype(jnp.float32) * LOG_DECAY)
    madv, mreach = mask_row * adv, mask_row * reach

    def add_up(a):
        return jnp.sum(a, axis=1, keepdims=True)

    carry_out = DISCOUNT * v_row[:, 0:1] + DECAY * adv[:, 0:1]
    parts = [add_up(mask_row), add_up(madv), add_up(madv * adv), add_up(mreach), add_up(mreach * adv), add_up(mreach * reach), carry_out]
    lane = lax.broadcasted_iota(jnp.int32, (1, 128), 1)
    packed = jnp.zeros((1, 128), jnp.float32)
    for place, part in enumerate(parts):
        packed = jnp.where(lane == place, part, packed)
    mine[...] = packed
    pair = pltpu.make_async_remote_copy(src_ref=mine, dst_ref=theirs, send_sem=pair_send, recv_sem=pair_recv,
                                        device_id=(chip, 1 - core), device_id_type=MESH)
    pair.start()
    pair.wait()
    other = theirs[...]
    is_left = core == 0
    left, right = jnp.where(is_left, packed, other), jnp.where(is_left, other, packed)
    carry = right[:, 6:7]
    count = left[:, 0:1] + right[:, 0:1]
    first = left[:, 1:2] + right[:, 1:2] + carry * left[:, 3:4]
    second = left[:, 2:3] + right[:, 2:3] + carry * (2.0 * left[:, 4:5] + carry * left[:, 5:6])
    own = jnp.where(lane == 0, count, jnp.where(lane == 1, first, jnp.where(lane == 2, second, 0.0)))
    total[...] = own

    def push(k, _):
        pltpu.make_async_remote_copy(
            src_ref=total, dst_ref=gathered.at[pl.ds(k - 1, 1)], send_sem=all_send, recv_sem=all_recv,
            device_id=(lax.rem(chip + k, dp_size), core), device_id_type=MESH).start()
        return 0

    lax.fori_loop(1, dp_size, push, 0)
    adv = adv + jnp.where(is_left, carry, 0.0) * reach
    out_ref[0:1, :] = v_row
    out_ref[1:2, :] = mask_row * (adv + v_row)
    everything = pltpu.make_async_remote_copy(src_ref=gathered, dst_ref=gathered, send_sem=all_send, recv_sem=all_recv,
                                              device_id=(chip, 1 - core), device_id_type=MESH)
    everything.wait_recv()
    sums = own + jnp.sum(gathered[...], axis=0, keepdims=True)
    count, first, second = sums[:, 0:1], sums[:, 1:2], sums[:, 2:3]
    mean = first / count
    var = second / count - mean * mean
    out_ref[2:3, :] = mask_row * (adv - mean) * lax.rsqrt(var + WHITEN_EPS)
    everything.wait_send()


def kernel(dp_size, x_hbm, wg, wu, wd, g2, gf, wv, bv, rew_ref, mask_ref, out_ref, weights_ref, reward_ref, *scratch):
    n = rew_ref.shape[1]
    mlp_scratch, tail_scratch = scratch[:13], scratch[13:]
    greet(dp_size)

    def while_loading():
        reward_ref[...] = reward_part(column_of(mask_ref[...].astype(jnp.float32) * rew_ref[...], n), n)
        weights_ref[...] = value_weights(n)

    mlp(x_hbm, wg, wu, wd, g2, gf, wv, *mlp_scratch, while_loading)
    model = x_hbm.shape[1]
    mask_row = mask_ref[...].astype(jnp.float32)
    sq_acc, hd_acc = mlp_scratch[6], mlp_scratch[7]
    square = jnp.sum(sq_acc[...], axis=1, keepdims=True)
    head = jnp.sum(hd_acc[...], axis=1, keepdims=True)
    v_col = column_of(mask_row, n) * (head * lax.rsqrt(square * (1.0 / model) + NORM_EPS) + bv[0])
    await_greetings(dp_size)
    finish(dp_size, v_col, reward_ref[...], weights_ref[...], mask_row, out_ref, *tail_scratch)


def hand_out(packed_ref, values_ref, returns_ref, white_ref):
    values_ref[...] = packed_ref[0:1, :]
    returns_ref[...] = packed_ref[1:2, :]
    white_ref[...] = packed_ref[2:3, :]


def mlp_scratch_shapes(rows, model, ffn):
    bf, f32, sem = jnp.bfloat16, jnp.float32, pltpu.SemaphoreType.DMA
    return [
        pltpu.VMEM((rows, model), bf),
        pltpu.VMEM((rows, model), bf),
        pltpu.VMEM((rows, ffn), bf),
        pltpu.VMEM((S1, model, WIDE), bf),
        pltpu.VMEM((S1, model, WIDE), bf),
        pltpu.VMEM((S2, DEPTH2, WIDE), bf),
        pltpu.VMEM((rows, 128), f32),
        pltpu.VMEM((rows, 128), f32),
        pltpu.VMEM((rows, WIDE), f32),
        sem, sem((S1,)), sem((S1,)), sem((S2,)),
    ]


def finish_scratch(dp_size):
    return [
        pltpu.VMEM((1, 128), jnp.float32),
        pltpu.VMEM((1, 128), jnp.float32),
        pltpu.VMEM((1, 128), jnp.float32),
        pltpu.VMEM((dp_size - 1, 128), jnp.float32),
        pltpu.SemaphoreType.DMA,
        pltpu.SemaphoreType.DMA,
        pltpu.SemaphoreType.DMA,
        pltpu.SemaphoreType.DMA,
    ]


def solution(mesh):
    dp_size = mesh.shape['dp']

    def local_step(x_blk, norm_gain, w_gate, w_up, w_down, final_gain, w_value, b_value, rew_blk, mask_blk):
        rows = rew_blk.shape[1]
        model, ffn = w_gate.shape
        hbm = pl.BlockSpec(memory_space=pl.ANY)
        vmem = pl.BlockSpec(memory_space=pltpu.VMEM)
        smem = pl.BlockSpec(memory_space=pltpu.SMEM)
        packed = pl.pallas_call(
            functools.partial(kernel, dp_size),
            out_shape=jax.ShapeDtypeStruct((8, rows), jnp.float32),
            in_specs=[hbm] * 4 + [vmem] * 3 + [smem] + [vmem] * 2,
            out_specs=vmem,
            scratch_shapes=[pltpu.VMEM((rows, rows), jnp.float32), pltpu.VMEM((1, rows), jnp.float32)]
            + mlp_scratch_shapes(rows, model, ffn) + finish_scratch(dp_size),
            compiler_params=pltpu.CompilerParams(collective_id=0, has_side_effects=True, vmem_limit_bytes=62 * 2**20),
        )(x_blk[0], w_gate, w_up, w_down, norm_gain[None], final_gain[None], w_value[None], b_value[None], rew_blk, mask_blk)
        row = jax.ShapeDtypeStruct((1, rows), jnp.float32)
        return pl.pallas_call(hand_out, out_shape=(row, row, row), in_specs=[vmem], out_specs=(vmem,) * 3)(packed)

    tok_spec = P('dp', 'cp')
    in_specs = (P('dp', 'cp', None), P(None), P(None, None), P(None, None), P(None, None), P(None), P(None), P(), tok_spec, tok_spec)
    return jax.shard_map(local_step, mesh=mesh, in_specs=in_specs, out_specs=(tok_spec, tok_spec, tok_spec), check_vma=False)
```

```python
import functools
import math

import jax
import jax.numpy as jnp
from jax import lax
from jax.experimental import pallas as pl
from jax.experimental.pallas import tpu as pltpu
from jax.sharding import PartitionSpec as P

NORM_EPS = 1e-6
WHITEN_EPS = 1e-8
DISCOUNT = 1.0
GAE_LAMBDA = 0.995
DECAY = DISCOUNT * GAE_LAMBDA
LOG_DECAY = math.log(DECAY)
MESH = pl.DeviceIdType.MESH


WIDE = 512
DEPTH2 = 2048
SLOTS = 3
AHEAD = 2
ALONE = 4


def silu_mul(g, u):
    return g * (1.0 / (1.0 + jnp.exp(-g))) * u


def dot(a, b):
    return jnp.dot(a, b, preferred_element_type=jnp.float32)


def mlp(dp_size, x_hbm, wg_hbm, wu_hbm, wd_hbm, g2_ref, gf_ref, wv_ref, rew_ref, mask_ref, weights_ref,
        x_buf, n_buf, n_stage, n_land, x_land, u_buf, u_stage, u_land, ring, h_buf, sq_acc, hd_acc, meta, meta_land,
        x_sem, ring_sem, n_send, n_recv, x_send, x_recv, meta_send, meta_recv, u_send, u_recv):
    rows, model = x_buf.shape
    ffn = u_buf.shape[1]
    chip, core = lax.axis_index("dp"), lax.axis_index("cp")
    chunks = ffn // WIDE
    shared = (chunks - ALONE) // 2
    out_cols = model // 2
    outs = out_cols // WIDE
    per_out = ffn // DEPTH2
    first2 = ALONE + shared
    steps = first2 + outs * per_out // 2

    def to_peer(src, dst, send, recv):
        return pltpu.make_async_remote_copy(src_ref=src, dst_ref=dst, send_sem=send, recv_sem=recv,
                                            device_id=(chip, 1 - core), device_id_type=MESH)

    def up_load(s, part, column):
        slot = lax.rem(s, SLOTS)
        src = (wg_hbm, wu_hbm)[part].at[:, pl.ds(pl.multiple_of(column * WIDE, WIDE), WIDE)]
        return pltpu.make_async_copy(src, ring.at[part, slot], ring_sem.at[part, slot])

    def column_at(s):
        if isinstance(s, int) and s < ALONE:
            return s
        return s + shared * core

    def down_load(s, part):
        slot = lax.rem(s, SLOTS)
        piece = (s - first2) * 2 + part
        o, j = piece // per_out, lax.rem(piece, per_out)
        src = wd_hbm.at[pl.ds(pl.multiple_of(depth_at(j) * DEPTH2, DEPTH2), DEPTH2),
                        pl.ds(pl.multiple_of(core * out_cols + o * WIDE, WIDE), WIDE)]
        return pltpu.make_async_copy(src, ring.at[part, slot, pl.ds(0, DEPTH2)], ring_sem.at[part, slot])

    def depth_at(j):
        turned = 1 + lax.rem(j + 2 + 2 * core, 3)
        if isinstance(j, int):
            return 0 if j == 0 else turned
        return jnp.where(j == 0, 0, turned)

    def start_load(s):
        for part in range(2):
            if s < first2:
                up_load(s, part, column_at(s)).start(priority=min(s, 1))
            else:
                down_load(s, part).start(priority=1)

    n_copy = to_peer(n_stage, n_land, n_send, n_recv)
    x_stage = n_stage.at[:, pl.ds(0, out_cols)]
    x_copy = to_peer(x_stage, x_land, x_send, x_recv)
    meta_copy = to_peer(meta, meta_land, meta_send, meta_recv)

    def u_copy(slot, unit):
        return to_peer(u_stage.at[slot], u_land.at[unit], u_send.at[slot], u_recv.at[unit])

    def take_unit(unit, block, column):
        u_copy(0, unit).wait_recv()
        u_buf[pl.ds(pl.multiple_of(block * rows, rows), rows), pl.ds(pl.multiple_of(column * WIDE, WIDE), WIDE)] = \
            u_land[unit].astype(jnp.bfloat16)

    own_x = pltpu.make_async_copy(x_hbm, x_buf, x_sem)
    own_x.start()
    for s in range(AHEAD):
        start_load(s)
    mask_row = mask_ref[...].astype(jnp.float32)
    meta[0:1, :] = reward_part(column_of(mask_row * rew_ref[...], rows), rows)
    meta[1:2, :] = mask_row
    weights_ref[...] = value_weights(rows)
    sq_acc[...] = jnp.zeros_like(sq_acc)
    hd_acc[...] = jnp.zeros_like(hd_acc)
    own_x.wait()

    def norm(b, _):
        r = pl.ds(pl.multiple_of(b * 32, 32), 32)
        xf = x_buf[r, :].astype(jnp.float32)
        scale = lax.rsqrt(jnp.mean(xf * xf, axis=1, keepdims=True) + NORM_EPS)
        normed = (xf * scale * g2_ref[...]).astype(jnp.bfloat16)
        n_buf[r, :] = normed
        n_stage[r, :] = normed.astype(jnp.float32)
        return 0

    lax.fori_loop(0, rows // 32, norm, 0)

    for s in range(ALONE):
        up_load(s, 0, column_at(s)).wait()
        start_load(s + AHEAD)
        gate = dot(n_buf[0:rows, :], ring[0, s % SLOTS])
        up_load(s, 1, column_at(s)).wait()
        hidden = silu_mul(gate, dot(n_buf[0:rows, :], ring[1, s % SLOTS])).astype(jnp.bfloat16)
        u_buf[0:rows, s * WIDE:(s + 1) * WIDE] = hidden
        u_stage[s] = hidden.astype(jnp.float32)
        if s == 0:
            await_greetings(dp_size)
            meta_copy.start()
            n_copy.start()
        u_copy(s, s).start()

    n_copy.wait_recv()
    n_buf[rows:2 * rows, :] = n_land[...].astype(jnp.bfloat16)
    n_copy.wait_send()
    x_stage[...] = x_buf[:, pl.ds(pl.multiple_of((1 - core) * out_cols, WIDE), out_cols)].astype(jnp.float32)
    x_copy.start()

    def both(b, _):
        for j in range(2):
            s = ALONE + 2 * b + j
            slot = lax.rem(s, SLOTS)
            column = column_at(s)
            for part in range(2):
                up_load(s, part, column).wait()
            @pl.when(s + AHEAD < first2)
            def _():
                for part in range(2):
                    up_load(s + AHEAD, part, column_at(s + AHEAD)).start(priority=1)

            @pl.when(s + AHEAD >= first2)
            def _():
                for part in range(2):
                    down_load(s + AHEAD, part).start(priority=1)
            for r in range(2):
                u_copy(2 * j + r, 0).wait_send()
            unit = 2 * b + j
            late = unit // ALONE
            take_unit(unit, 1 - lax.rem(unit, 2) * late, (1 - late) * unit + late * (ALONE + shared * (1 - core)))
            half = WIDE // 2
            for q in range(2):
                c = pl.ds(q * half, half)
                hidden = silu_mul(dot(n_buf[...], ring[0, slot, :, c]), dot(n_buf[...], ring[1, slot, :, c])).astype(jnp.bfloat16)
                u_buf[:, pl.ds(pl.multiple_of(column * WIDE + q * half, half), half)] = hidden
                wide = hidden.astype(jnp.float32)
                for r in range(2):
                    u_stage[2 * j + r, :, c] = wide[r * rows:(r + 1) * rows]
            for r in range(2):
                u_copy(2 * j + r, ALONE + 2 * (s - ALONE) + r).start()

        return 0

    lax.fori_loop(0, shared // 2, both, 0)

    def take_late(unit):
        take_unit(unit, 1 - unit % 2, ALONE + shared * (1 - core) + (unit - ALONE) // 2)

    def load_more(o, s):
        if isinstance(o, int):
            start_load(s)
        else:
            @pl.when(s < steps)
            def _():
                for part in range(2):
                    down_load(s, part).start(priority=1)

    def out_tile(o, starting):
        for j in range(per_out):
            s = first2 + 2 * o + j // 2
            slot, part = lax.rem(s, SLOTS), j % 2
            down_load(s, part).wait()
            if part == 0:
                load_more(o, s + AHEAD)
            if starting and j < 3:
                for unit in ((6, 7, 8, 9), (10, 11, 12, 13), (14, 15))[j]:
                    take_late(unit)
            if starting and j == 3:
                x_copy.wait_recv()
            lhs = u_buf[:, pl.ds(pl.multiple_of(depth_at(j) * DEPTH2, DEPTH2), DEPTH2)]
            if j < per_out - 1:
                value = dot(lhs, ring[part, slot, 0:DEPTH2])
                h_buf[...] = value if j == 0 else h_buf[...] + value
            else:
                half = WIDE // 2
                for q in range(2):
                    value = h_buf[:, q * half:(q + 1) * half] + dot(lhs, ring[part, slot, 0:DEPTH2, q * half:(q + 1) * half])
                    own = pl.ds(pl.multiple_of(core * out_cols + o * WIDE + q * half, half), half)
                    there = pl.ds(pl.multiple_of(o * WIDE + q * half, half), half)
                    head = gf_ref[:, own] * wv_ref[:, own]
                    for r, resid in enumerate((x_buf[:, own].astype(jnp.float32), x_land[:, there])):
                        block = slice(r * rows, (r + 1) * rows)
                        h = resid + value[block]
                        sq, hd = h * h, h * head
                        sq_acc[block, :] += sq[:, :128] + sq[:, 128:]
                        hd_acc[block, :] += hd[:, :128] + hd[:, 128:]

    out_tile(0, True)

    def rest(o, _):
        out_tile(o, False)
        return 0

    lax.fori_loop(1, outs, rest, 0)
    for slot in range(4):
        u_copy(slot, 0).wait_send()
    x_copy.wait_send()
    meta_copy.wait()


def greet(dp_size):
    chip, core = lax.axis_index("dp"), lax.axis_index("cp")
    barrier = pltpu.get_barrier_semaphore()
    pl.semaphore_signal(barrier, inc=1, device_id=(chip, 1 - core), device_id_type=MESH)

    def tell(k, _):
        pl.semaphore_signal(barrier, inc=1, device_id=(lax.rem(chip + k, dp_size), core), device_id_type=MESH)
        return 0

    lax.fori_loop(1, dp_size, tell, 0)


def await_greetings(dp_size):
    pl.semaphore_wait(pltpu.get_barrier_semaphore(), dp_size)


def positions(n):
    row = lax.broadcasted_iota(jnp.int32, (n, n), 0)
    col = lax.broadcasted_iota(jnp.int32, (n, n), 1)
    return row, col


def column_of(row_vec, n):
    row, col = positions(n)
    return jnp.sum(jnp.where(row == col, row_vec, 0.0), axis=1, keepdims=True)


def reward_part(rew_col, n):
    row, col = positions(n)
    gap = row - col
    decay = jnp.where(gap >= 0, jnp.exp(jnp.maximum(gap, 0).astype(jnp.float32) * LOG_DECAY), 0.0)
    return jnp.sum(decay * rew_col, axis=0, keepdims=True)


def value_weights(n):
    row, col = positions(n)
    gap = row - col
    later = DISCOUNT * (1.0 - GAE_LAMBDA) * jnp.exp(jnp.maximum(gap - 1, 0).astype(jnp.float32) * LOG_DECAY)
    return jnp.where(gap > 0, later, jnp.where(gap == 0, -1.0, 0.0))


def finish(dp_size, bv, model, weights_ref, sq_acc, hd_acc, meta, meta_land, out_ref,
           mine, theirs, total, gathered, pair_send, pair_recv, all_send, all_recv):
    n = meta.shape[1]
    chip, core = lax.axis_index("dp"), lax.axis_index("cp")
    row, col = positions(n)

    def to_row(col_vec):
        return jnp.sum(jnp.where(row == col, col_vec, 0.0), axis=0, keepdims=True)

    for r in range(2):
        block = slice(r * n, (r + 1) * n)
        mine[2 * r:2 * r + 1, :] = to_row(jnp.sum(sq_acc[block, :], axis=1, keepdims=True))
        mine[2 * r + 1:2 * r + 2, :] = to_row(jnp.sum(hd_acc[block, :], axis=1, keepdims=True))
    pair = pltpu.make_async_remote_copy(src_ref=mine, dst_ref=theirs, send_sem=pair_send, recv_sem=pair_recv,
                                        device_id=(chip, 1 - core), device_id_type=MESH)
    pair.start()
    own_mask, other_mask = meta[1:2, :], meta_land[1:2, :]
    is_left = core == 0
    ahead = (n - 1) - lax.broadcasted_iota(jnp.int32, (1, n), 1)
    reach = jnp.exp(ahead.astype(jnp.float32) * LOG_DECAY)
    pair.wait()

    def value(r, mask):
        square = mine[2 * r:2 * r + 1, :] + theirs[2 - 2 * r:3 - 2 * r, :]
        head = mine[2 * r + 1:2 * r + 2, :] + theirs[3 - 2 * r:4 - 2 * r, :]
        return mask * (head * lax.rsqrt(square * (1.0 / model) + NORM_EPS) + bv)

    own_v, other_v = value(0, own_mask), value(1, other_mask)
    weights = weights_ref[...]

    def local_adv(v, reward_row):
        return reward_row + jnp.sum(weights * column_of(v, n), axis=0, keepdims=True)

    own_adv, other_adv = local_adv(own_v, meta[0:1, :]), local_adv(other_v, meta_land[0:1, :])
    right_v = jnp.where(is_left, other_v, own_v)
    right_adv = jnp.where(is_left, other_adv, own_adv)
    carry = DISCOUNT * right_v[:, 0:1] + DECAY * right_adv[:, 0:1]
    own_adv = own_adv + jnp.where(is_left, carry, 0.0) * reach
    other_adv = other_adv + jnp.where(is_left, 0.0, carry) * reach
    own_m, other_m = own_mask * own_adv, other_mask * other_adv

    def add_up(a):
        return jnp.sum(a, axis=1, keepdims=True)

    parts = (add_up(own_mask + other_mask), add_up(own_m + other_m), add_up(own_m * own_adv + other_m * other_adv))
    lane = lax.broadcasted_iota(jnp.int32, (1, 128), 1)
    own = jnp.zeros((1, 128), jnp.float32)
    for place, part in enumerate(parts):
        own = jnp.where(lane == place, part, own)
    total[...] = own

    def push(k, _):
        pltpu.make_async_remote_copy(
            src_ref=total, dst_ref=gathered.at[pl.ds(k - 1, 1)], send_sem=all_send, recv_sem=all_recv,
            device_id=(lax.rem(chip + k, dp_size), core), device_id_type=MESH).start()
        return 0

    lax.fori_loop(1, dp_size, push, 0)
    out_ref[0:1, :] = own_v
    out_ref[1:2, :] = own_mask * (own_adv + own_v)
    everything = pltpu.make_async_remote_copy(src_ref=gathered, dst_ref=gathered, send_sem=all_send, recv_sem=all_recv,
                                              device_id=(chip, 1 - core), device_id_type=MESH)
    everything.wait_recv()
    sums = own + jnp.sum(gathered[...], axis=0, keepdims=True)
    count, first, second = sums[:, 0:1], sums[:, 1:2], sums[:, 2:3]
    mean = first / count
    var = second / count - mean * mean
    out_ref[2:3, :] = own_mask * (own_adv - mean) * lax.rsqrt(var + WHITEN_EPS)
    everything.wait_send()


def kernel(dp_size, x_hbm, wg, wu, wd, g2, gf, wv, bv, rew_ref, mask_ref, out_ref, weights_ref, *scratch):
    mlp_scratch, tail_scratch = scratch[:24], scratch[24:]
    greet(dp_size)
    mlp(dp_size, x_hbm, wg, wu, wd, g2, gf, wv, rew_ref, mask_ref, weights_ref, *mlp_scratch)
    finish(dp_size, bv[0], x_hbm.shape[1], weights_ref, *mlp_scratch[10:14], out_ref, *tail_scratch)


def hand_out(packed_ref, values_ref, returns_ref, white_ref):
    values_ref[...] = packed_ref[0:1, :]
    returns_ref[...] = packed_ref[1:2, :]
    white_ref[...] = packed_ref[2:3, :]


def scratch_shapes(dp_size, rows, model, ffn):
    bf, f32, sem = jnp.bfloat16, jnp.float32, pltpu.SemaphoreType.DMA
    vmem = pltpu.VMEM
    units = ALONE + (ffn // WIDE - ALONE)
    return [
        vmem((rows, rows), f32),
        vmem((rows, model), bf),
        vmem((2 * rows, model), bf),
        vmem((rows, model), f32),
        vmem((rows, model), f32),
        vmem((rows, model // 2), f32),
        vmem((2 * rows, ffn), bf),
        vmem((4, rows, WIDE), f32),
        vmem((units, rows, WIDE), f32),
        vmem((2, SLOTS, model, WIDE), bf),
        vmem((2 * rows, WIDE), f32),
        vmem((2 * rows, 128), f32),
        vmem((2 * rows, 128), f32),
        vmem((8, rows), f32),
        vmem((8, rows), f32),
        sem, sem((2, SLOTS)), sem, sem, sem, sem, sem, sem, sem((4,)), sem((units,)),
        vmem((8, rows), f32),
        vmem((8, rows), f32),
        vmem((1, 128), f32),
        vmem((dp_size - 1, 128), f32),
        sem, sem, sem, sem,
    ]


def solution(mesh):
    dp_size = mesh.shape['dp']

    def local_step(x_blk, norm_gain, w_gate, w_up, w_down, final_gain, w_value, b_value, rew_blk, mask_blk):
        rows = rew_blk.shape[1]
        model, ffn = w_gate.shape
        hbm = pl.BlockSpec(memory_space=pl.ANY)
        vmem = pl.BlockSpec(memory_space=pltpu.VMEM)
        smem = pl.BlockSpec(memory_space=pltpu.SMEM)
        packed = pl.pallas_call(
            functools.partial(kernel, dp_size),
            out_shape=jax.ShapeDtypeStruct((8, rows), jnp.float32),
            in_specs=[hbm] * 4 + [vmem] * 3 + [smem] + [vmem] * 2,
            out_specs=vmem,
            scratch_shapes=scratch_shapes(dp_size, rows, model, ffn),
            compiler_params=pltpu.CompilerParams(collective_id=0, has_side_effects=True, vmem_limit_bytes=63 * 2**20),
        )(x_blk[0], w_gate, w_up, w_down, norm_gain[None], final_gain[None], w_value[None], b_value[None], rew_blk, mask_blk)
        row = jax.ShapeDtypeStruct((1, rows), jnp.float32)
        return pl.pallas_call(hand_out, out_shape=(row, row, row), in_specs=[vmem], out_specs=(vmem,) * 3)(packed)

    tok_spec = P('dp', 'cp')
    in_specs = (P('dp', 'cp', None), P(None), P(None, None), P(None, None), P(None, None), P(None), P(None), P(), tok_spec, tok_spec)
    return jax.shard_map(local_step, mesh=mesh, in_specs=in_specs, out_specs=(tok_spec, tok_spec, tok_spec), check_vma=False)
```

```python
import functools
import math

import jax
import jax.numpy as jnp
from jax import lax
from jax.experimental import pallas as pl
from jax.experimental.pallas import tpu as pltpu
from jax.sharding import PartitionSpec as P

NORM_EPS = 1e-6
WHITEN_EPS = 1e-8
DISCOUNT = 1.0
GAE_LAMBDA = 0.995
DECAY = DISCOUNT * GAE_LAMBDA
LOG_DECAY = math.log(DECAY)
MESH = pl.DeviceIdType.MESH


WIDE = 512
DEPTH2 = 2048
SLOTS = 3
AHEAD = 2
SPLIT = 1
SPLIT2 = 1
FIRST = 1
EAGER = 2
ALONE = 4


def silu_mul(g, u):
    return g * (1.0 / (1.0 + jnp.exp(-g))) * u


def dot(a, b):
    return jnp.dot(a, b, preferred_element_type=jnp.float32)


def mlp(dp_size, x_hbm, wg_hbm, wu_hbm, wd_hbm, g2_ref, gf_ref, wv_ref, rew_ref, mask_ref, weights_ref,
        x_buf, n_buf, n_stage, n_land, x_land, u_buf, u_stage, u_land, ring, h_buf, sq_acc, hd_acc, meta, meta_land,
        x_sem, ring_sem, n_send, n_recv, x_send, x_recv, meta_send, meta_recv, u_send, u_recv):
    rows, model = x_buf.shape
    ffn = u_buf.shape[1]
    chip, core = lax.axis_index("dp"), lax.axis_index("cp")
    chunks = ffn // WIDE
    shared = (chunks - ALONE) // 2
    out_cols = model // 2
    outs = out_cols // WIDE
    per_out = ffn // DEPTH2
    first2 = ALONE + shared
    steps = first2 + outs * per_out // 2

    def to_peer(src, dst, send, recv):
        return pltpu.make_async_remote_copy(src_ref=src, dst_ref=dst, send_sem=send, recv_sem=recv,
                                            device_id=(chip, 1 - core), device_id_type=MESH)

    def up_load(s, part, column, rows_from=0, row_count=model):
        slot, r = lax.rem(s, SLOTS), pl.ds(rows_from, row_count)
        src = (wg_hbm, wu_hbm)[part].at[r, pl.ds(pl.multiple_of(column * WIDE, WIDE), WIDE)]
        return pltpu.make_async_copy(src, ring.at[part, slot, r], ring_sem.at[part, slot])

    def column_at(s):
        if isinstance(s, int) and s < ALONE:
            return s
        return s + shared * core

    def down_load(s, part, rows_from=0, row_count=DEPTH2):
        slot = lax.rem(s, SLOTS)
        piece = (s - first2) * 2 + part
        o, j = piece // per_out, lax.rem(piece, per_out)
        src = wd_hbm.at[pl.ds(pl.multiple_of(depth_at(j) * DEPTH2 + rows_from, row_count), row_count),
                        pl.ds(pl.multiple_of(core * out_cols + o * WIDE, WIDE), WIDE)]
        return pltpu.make_async_copy(src, ring.at[part, slot, pl.ds(rows_from, row_count)], ring_sem.at[part, slot])

    def depth_at(j):
        turned = 1 + lax.rem(j + 2 + 2 * core, 3)
        if isinstance(j, int):
            return 0 if j == 0 else turned
        return jnp.where(j == 0, 0, turned)

    def start_up(s):
        for part in range(2):
            for i in range(SPLIT):
                up_load(s, part, column_at(s), i * (model // SPLIT), model // SPLIT).start(priority=FIRST)

    def start_down(s):
        for part in range(2):
            for i in range(SPLIT2):
                down_load(s, part, i * (DEPTH2 // SPLIT2), DEPTH2 // SPLIT2).start(priority=FIRST)

    def start_load(s):
        if s < first2:
            start_up(s)
        else:
            start_down(s)

    n_copy = to_peer(n_stage, n_land, n_send, n_recv)
    x_stage = n_stage.at[:, pl.ds(0, out_cols)]
    x_copy = to_peer(x_stage, x_land, x_send, x_recv)
    meta_copy = to_peer(meta, meta_land, meta_send, meta_recv)

    def u_copy(slot, unit):
        return to_peer(u_stage.at[slot], u_land.at[unit], u_send.at[slot], u_recv.at[unit])

    def take_unit(unit, block, column):
        u_copy(0, unit).wait_recv()
        u_buf[pl.ds(pl.multiple_of(block * rows, rows), rows), pl.ds(pl.multiple_of(column * WIDE, WIDE), WIDE)] = \
            u_land[unit].astype(jnp.bfloat16)

    own_x = pltpu.make_async_copy(x_hbm, x_buf, x_sem)
    own_x.start()
    for s in range(EAGER):
        start_load(s)
    mask_row = mask_ref[...].astype(jnp.float32)
    meta[0:1, :] = reward_part(column_of(mask_row * rew_ref[...], rows), rows)
    meta[1:2, :] = mask_row
    weights_ref[...] = value_weights(rows)
    sq_acc[...] = jnp.zeros_like(sq_acc)
    hd_acc[...] = jnp.zeros_like(hd_acc)
    own_x.wait()

    def norm(b, _):
        r = pl.ds(pl.multiple_of(b * 32, 32), 32)
        xf = x_buf[r, :].astype(jnp.float32)
        scale = lax.rsqrt(jnp.mean(xf * xf, axis=1, keepdims=True) + NORM_EPS)
        normed = (xf * scale * g2_ref[...]).astype(jnp.bfloat16)
        n_buf[r, :] = normed
        n_stage[r, :] = normed.astype(jnp.float32)
        return 0

    lax.fori_loop(0, rows // 32, norm, 0)

    await_greetings(dp_size)
    meta_copy.start()
    n_copy.start()

    for s in range(ALONE):
        up_load(s, 0, column_at(s)).wait()
        if s + AHEAD >= EAGER:
            start_load(s + AHEAD)
        gate = dot(n_buf[0:rows, :], ring[0, s % SLOTS])
        up_load(s, 1, column_at(s)).wait()
        if s == ALONE - 1:
            n_copy.wait_recv()
            n_buf[rows:2 * rows, :] = n_land[...].astype(jnp.bfloat16)
            n_copy.wait_send()
            x_stage[...] = x_buf[:, pl.ds(pl.multiple_of((1 - core) * out_cols, WIDE), out_cols)].astype(jnp.float32)
        hidden = silu_mul(gate, dot(n_buf[0:rows, :], ring[1, s % SLOTS])).astype(jnp.bfloat16)
        u_buf[0:rows, s * WIDE:(s + 1) * WIDE] = hidden
        u_stage[s] = hidden.astype(jnp.float32)
        u_copy(s, s).start()

    x_copy.start()

    def both(b, _):
        for j in range(2):
            s = ALONE + 2 * b + j
            slot = lax.rem(s, SLOTS)
            column = column_at(s)
            for part in range(2):
                up_load(s, part, column).wait()
            @pl.when(s + AHEAD < first2)
            def _():
                start_up(s + AHEAD)

            @pl.when(s + AHEAD >= first2)
            def _():
                start_down(s + AHEAD)
            for r in range(2):
                u_copy(2 * j + r, 0).wait_send()
            unit = 2 * b + j
            late = unit // ALONE
            take_unit(unit, 1 - lax.rem(unit, 2) * late, (1 - late) * unit + late * (ALONE + shared * (1 - core)))
            half = WIDE // 2
            for q in range(2):
                c = pl.ds(q * half, half)
                hidden = silu_mul(dot(n_buf[...], ring[0, slot, :, c]), dot(n_buf[...], ring[1, slot, :, c])).astype(jnp.bfloat16)
                u_buf[:, pl.ds(pl.multiple_of(column * WIDE + q * half, half), half)] = hidden
                wide = hidden.astype(jnp.float32)
                for r in range(2):
                    u_stage[2 * j + r, :, c] = wide[r * rows:(r + 1) * rows]
            for r in range(2):
                u_copy(2 * j + r, ALONE + 2 * (s - ALONE) + r).start()

        return 0

    lax.fori_loop(0, shared // 2, both, 0)

    def take_late(unit):
        take_unit(unit, 1 - unit % 2, ALONE + shared * (1 - core) + (unit - ALONE) // 2)

    def out_tile(o, starting):
        for j in range(per_out):
            s = first2 + 2 * o + j // 2
            slot, part = lax.rem(s, SLOTS), j % 2
            down_load(s, part).wait()
            if part == 0 and s + AHEAD < steps:
                start_load(s + AHEAD)
            if starting and j < 3:
                for unit in ((6, 7, 8, 9), (10, 11, 12, 13), (14, 15))[j]:
                    take_late(unit)
            if starting and j == 3:
                x_copy.wait_recv()
            lhs = u_buf[:, pl.ds(pl.multiple_of(depth_at(j) * DEPTH2, DEPTH2), DEPTH2)]
            if j < per_out - 1:
                value = dot(lhs, ring[part, slot, 0:DEPTH2])
                h_buf[...] = value if j == 0 else h_buf[...] + value
            else:
                half = WIDE // 2
                for q in range(2):
                    value = h_buf[:, q * half:(q + 1) * half] + dot(lhs, ring[part, slot, 0:DEPTH2, q * half:(q + 1) * half])
                    own = pl.ds(pl.multiple_of(core * out_cols + o * WIDE + q * half, half), half)
                    there = pl.ds(pl.multiple_of(o * WIDE + q * half, half), half)
                    head = gf_ref[:, own] * wv_ref[:, own]
                    for r, resid in enumerate((x_buf[:, own].astype(jnp.float32), x_land[:, there])):
                        block = slice(r * rows, (r + 1) * rows)
                        h = resid + value[block]
                        sq, hd = h * h, h * head
                        sq_acc[block, :] += sq[:, :128] + sq[:, 128:]
                        hd_acc[block, :] += hd[:, :128] + hd[:, 128:]

    for o in range(outs):
        out_tile(o, o == 0)
    for slot in range(4):
        u_copy(slot, 0).wait_send()
    x_copy.wait_send()
    meta_copy.wait()


def greet(dp_size):
    chip, core = lax.axis_index("dp"), lax.axis_index("cp")
    barrier = pltpu.get_barrier_semaphore()
    pl.semaphore_signal(barrier, inc=1, device_id=(chip, 1 - core), device_id_type=MESH)

    def tell(k, _):
        pl.semaphore_signal(barrier, inc=1, device_id=(lax.rem(chip + k, dp_size), core), device_id_type=MESH)
        return 0

    lax.fori_loop(1, dp_size, tell, 0)


def await_greetings(dp_size):
    pl.semaphore_wait(pltpu.get_barrier_semaphore(), dp_size)


def positions(n):
    row = lax.broadcasted_iota(jnp.int32, (n, n), 0)
    col = lax.broadcasted_iota(jnp.int32, (n, n), 1)
    return row, col


def column_of(row_vec, n):
    row, col = positions(n)
    return jnp.sum(jnp.where(row == col, row_vec, 0.0), axis=1, keepdims=True)


def reward_part(rew_col, n):
    row, col = positions(n)
    gap = row - col
    decay = jnp.where(gap >= 0, jnp.exp(jnp.maximum(gap, 0).astype(jnp.float32) * LOG_DECAY), 0.0)
    return jnp.sum(decay * rew_col, axis=0, keepdims=True)


def value_weights(n):
    row, col = positions(n)
    gap = row - col
    later = DISCOUNT * (1.0 - GAE_LAMBDA) * jnp.exp(jnp.maximum(gap - 1, 0).astype(jnp.float32) * LOG_DECAY)
    return jnp.where(gap > 0, later, jnp.where(gap == 0, -1.0, 0.0))


def others(chip, dp_size):
    side = round(dp_size ** (1 / 3))
    if side ** 3 != dp_size:
        return [lax.rem(chip + k, dp_size) for k in range(1, dp_size)]
    coords = [lax.rem(chip // side ** i, side) for i in range(3)]
    shifted = [[lax.rem(c + d, side) * side ** i for d in range(side)] for i, c in enumerate(coords)]
    steps = sorted(((min(x, side - x) + min(y, side - y) + min(z, side - z)), x, y, z)
                   for x in range(side) for y in range(side) for z in range(side))
    return [shifted[0][x] + shifted[1][y] + shifted[2][z] for _, x, y, z in steps[:0:-1]]


def finish(dp_size, bv, model, weights_ref, sq_acc, hd_acc, meta, meta_land, out_ref,
           mine, theirs, total, gathered, pair_send, pair_recv, all_send, all_recv):
    n = meta.shape[1]
    chip, core = lax.axis_index("dp"), lax.axis_index("cp")
    row, col = positions(n)

    def to_row(col_vec):
        return jnp.sum(jnp.where(row == col, col_vec, 0.0), axis=0, keepdims=True)

    for r in range(2):
        block = slice(r * n, (r + 1) * n)
        mine[2 * r:2 * r + 1, :] = to_row(jnp.sum(sq_acc[block, :], axis=1, keepdims=True))
        mine[2 * r + 1:2 * r + 2, :] = to_row(jnp.sum(hd_acc[block, :], axis=1, keepdims=True))
    pair = pltpu.make_async_remote_copy(src_ref=mine, dst_ref=theirs, send_sem=pair_send, recv_sem=pair_recv,
                                        device_id=(chip, 1 - core), device_id_type=MESH)
    pair.start()
    own_mask, other_mask = meta[1:2, :], meta_land[1:2, :]
    is_left = core == 0
    ahead = (n - 1) - lax.broadcasted_iota(jnp.int32, (1, n), 1)
    reach = jnp.exp(ahead.astype(jnp.float32) * LOG_DECAY)
    pair.wait()

    def value(r, mask):
        square = mine[2 * r:2 * r + 1, :] + theirs[2 - 2 * r:3 - 2 * r, :]
        head = mine[2 * r + 1:2 * r + 2, :] + theirs[3 - 2 * r:4 - 2 * r, :]
        return mask * (head * lax.rsqrt(square * (1.0 / model) + NORM_EPS) + bv)

    own_v, other_v = value(0, own_mask), value(1, other_mask)
    weights = weights_ref[...]

    def local_adv(v, reward_row):
        return reward_row + jnp.sum(weights * column_of(v, n), axis=0, keepdims=True)

    own_adv, other_adv = local_adv(own_v, meta[0:1, :]), local_adv(other_v, meta_land[0:1, :])
    right_v = jnp.where(is_left, other_v, own_v)
    right_adv = jnp.where(is_left, other_adv, own_adv)
    carry = DISCOUNT * right_v[:, 0:1] + DECAY * right_adv[:, 0:1]
    own_adv = own_adv + jnp.where(is_left, carry, 0.0) * reach
    other_adv = other_adv + jnp.where(is_left, 0.0, carry) * reach
    own_m, other_m = own_mask * own_adv, other_mask * other_adv

    def add_up(a):
        return jnp.sum(a, axis=1, keepdims=True)

    parts = (add_up(own_mask + other_mask), add_up(own_m + other_m), add_up(own_m * own_adv + other_m * other_adv))
    lane = lax.broadcasted_iota(jnp.int32, (1, 128), 1)
    own = jnp.zeros((1, 128), jnp.float32)
    for place, part in enumerate(parts):
        own = jnp.where(lane == place, part, own)
    total[...] = own

    for k, there in enumerate(others(chip, dp_size)):
        pltpu.make_async_remote_copy(
            src_ref=total, dst_ref=gathered.at[pl.ds(k, 1)], send_sem=all_send, recv_sem=all_recv,
            device_id=(there, core), device_id_type=MESH).start()
    out_ref[0:1, :] = own_v
    out_ref[1:2, :] = own_mask * (own_adv + own_v)
    everything = pltpu.make_async_remote_copy(src_ref=gathered, dst_ref=gathered, send_sem=all_send, recv_sem=all_recv,
                                              device_id=(chip, 1 - core), device_id_type=MESH)
    everything.wait_recv()
    sums = own + jnp.sum(gathered[...], axis=0, keepdims=True)
    count, first, second = sums[:, 0:1], sums[:, 1:2], sums[:, 2:3]
    mean = first / count
    var = second / count - mean * mean
    out_ref[2:3, :] = own_mask * (own_adv - mean) * lax.rsqrt(var + WHITEN_EPS)
    everything.wait_send()


def kernel(dp_size, x_hbm, wg, wu, wd, g2, gf, wv, bv, rew_ref, mask_ref, out_ref, weights_ref, *scratch):
    mlp_scratch, tail_scratch = scratch[:24], scratch[24:]
    greet(dp_size)
    mlp(dp_size, x_hbm, wg, wu, wd, g2, gf, wv, rew_ref, mask_ref, weights_ref, *mlp_scratch)
    finish(dp_size, bv[0], x_hbm.shape[1], weights_ref, *mlp_scratch[10:14], out_ref, *tail_scratch)


def hand_out(packed_ref, values_ref, returns_ref, white_ref):
    values_ref[...] = packed_ref[0:1, :]
    returns_ref[...] = packed_ref[1:2, :]
    white_ref[...] = packed_ref[2:3, :]


def scratch_shapes(dp_size, rows, model, ffn):
    bf, f32, sem = jnp.bfloat16, jnp.float32, pltpu.SemaphoreType.DMA
    vmem = pltpu.VMEM
    units = ALONE + (ffn // WIDE - ALONE)
    return [
        vmem((rows, rows), f32),
        vmem((rows, model), bf),
        vmem((2 * rows, model), bf),
        vmem((rows, model), f32),
        vmem((rows, model), f32),
        vmem((rows, model // 2), f32),
        vmem((2 * rows, ffn), bf),
        vmem((4, rows, WIDE), f32),
        vmem((units, rows, WIDE), f32),
        vmem((2, SLOTS, model, WIDE), bf),
        vmem((2 * rows, WIDE), f32),
        vmem((2 * rows, 128), f32),
        vmem((2 * rows, 128), f32),
        vmem((8, rows), f32),
        vmem((8, rows), f32),
        sem, sem((2, SLOTS)), sem, sem, sem, sem, sem, sem, sem((4,)), sem((units,)),
        vmem((8, rows), f32),
        vmem((8, rows), f32),
        vmem((1, 128), f32),
        vmem((dp_size - 1, 128), f32),
        sem, sem, sem, sem,
    ]


def solution(mesh):
    dp_size = mesh.shape['dp']

    def local_step(x_blk, norm_gain, w_gate, w_up, w_down, final_gain, w_value, b_value, rew_blk, mask_blk):
        rows = rew_blk.shape[1]
        model, ffn = w_gate.shape
        hbm = pl.BlockSpec(memory_space=pl.ANY)
        vmem = pl.BlockSpec(memory_space=pltpu.VMEM)
        smem = pl.BlockSpec(memory_space=pltpu.SMEM)
        packed = pl.pallas_call(
            functools.partial(kernel, dp_size),
            out_shape=jax.ShapeDtypeStruct((8, rows), jnp.float32),
            in_specs=[hbm] * 4 + [vmem] * 3 + [smem] + [vmem] * 2,
            out_specs=vmem,
            scratch_shapes=scratch_shapes(dp_size, rows, model, ffn),
            compiler_params=pltpu.CompilerParams(collective_id=0, has_side_effects=True, vmem_limit_bytes=63 * 2**20),
        )(x_blk[0], w_gate, w_up, w_down, norm_gain[None], final_gain[None], w_value[None], b_value[None], rew_blk, mask_blk)
        row = jax.ShapeDtypeStruct((1, rows), jnp.float32)
        return pl.pallas_call(hand_out, out_shape=(row, row, row), in_specs=[vmem], out_specs=(vmem,) * 3)(packed)

    tok_spec = P('dp', 'cp')
    in_specs = (P('dp', 'cp', None), P(None), P(None, None), P(None, None), P(None, None), P(None), P(None), P(), tok_spec, tok_spec)
    return jax.shard_map(local_step, mesh=mesh, in_specs=in_specs, out_specs=(tok_spec, tok_spec, tok_spec), check_vma=False)
```
